32 devices in a mesh: seq: 8 (over z, x), batch: 4 (over y, core).
Axes of the slice: x: 2, y: 2, z: 4, core: 2. Of those that a mesh axis runs over, the one named last changes fastest.
Arguments:
- hidden: bfloat16 [8, 2048, 4096], P('batch', None, 'seq')
- gain: float32 [4096], P('seq'), may hold values from 0.5 to 1.5
- value_weight: float32 [4096], P('seq'), may hold values from -0.09375 to 0.09375
- rewards: float32 [8, 2048], P('batch', 'seq'), may hold values from -1.5 to 1.5
- reward_mask: int32 [8, 2048], P('batch', 'seq'), may hold values 0 or 1
- lengths: int32 [8], P('batch'), may hold values from 512 to 2048
- horizon: float32 [8], P('batch'), may hold values from 24 to 16384
Outputs:
- advantages: float32 [8, 2048], P(None, ('seq', 'batch'))
- returns: float32 [8, 2048], P(None, ('seq', 'batch'))
The draws below stay inside these ranges and needn't reach their ends.
All inputs are finite; a program needn't handle non-finite values. No bound on the sum of `reward_mask` on one device may be relied on, other than what follows from the above.
Results may differ from the reference program's by a relative error of at most 0.0003.
Values may be sent and summed in bfloat16 or wider, within the bound.
No kernel may reach another device: no remote copies, remote signals or barrier semaphores. Data moves between devices by JAX's collectives and lax.ppermute only.
A program may use at most 64 MiB of HBM per device.

```python
import jax
import jax.numpy as jnp
from jax import lax

D = 4096
B = 8
S = 2048


def draw_hidden(key, part):
    first_key = jax.random.fold_in(key, 11)
    second_key = jax.random.fold_in(key, 12)
    base = jax.random.normal(first_key, (B, S, D), jnp.float32)
    scales = jnp.exp(jax.random.uniform(second_key, (B, S, D // 16, 1), jnp.float32, -1.2, 1.2))
    return (base.reshape(B, S, D // 16, 16) * scales).reshape(B, S, D).astype(jnp.bfloat16)


def draw_horizon(key, part):
    inner = jax.random.fold_in(key, 21)
    lower = jnp.log(24.0)
    upper = jnp.log(4.0 * S)
    return jnp.exp(jax.random.uniform(inner, (B,), jnp.float32, lower, upper)).astype(jnp.float32)


def place_ends(drawn, rng, least, high):
    dims = drawn.shape
    index_at = [jax.random.randint(jax.random.fold_in(rng, axis), (), 0, dims[axis]) for axis in range(len(dims))]
    drawn = drawn.at[tuple(index_at)].set(least)
    longest = dims.index(max(dims))
    index_at[longest] = (index_at[longest] + 1) % dims[longest]
    return drawn.at[tuple(index_at)].set(high)


def level_of(key, dims, shards, low, high):
    factor_of = 1.0
    for axis_at, parts in shards:
        steps = jax.random.uniform(jax.random.fold_in(jax.random.fold_in(key, 6), axis_at), (parts,), jnp.float32, low / len(shards), high / len(shards))
        factor_of = factor_of * jnp.repeat(jnp.exp(steps), dims[axis_at] // parts).reshape((-1,) + (1,) * (len(dims) - 1 - axis_at))
    return factor_of


def normal_values(own_key, dims, scale, limit, split=(), held_as=jnp.bfloat16):
    result = scale * jax.random.normal(own_key, dims, jnp.float32)
    if split:
        result = result * level_of(own_key, dims, split, -0.22, 0.18)
    return jnp.clip(result, -limit, limit).astype(held_as)


def setup_inputs(seed: int = 0) -> dict:
    splits = jax.random.split(jax.random.key(seed), 8)
    return {
        "hidden": draw_hidden(jax.random.fold_in(splits[7], 71), 0),
        "gain": jnp.clip(1.0 + 0.1 * jax.random.normal(splits[1], (D,), jnp.float32), 0.5, 1.5),
        "value_weight": normal_values(splits[2], (D,), D ** -0.5, 0.09375, ((0, 8),), jnp.float32),
        "rewards": normal_values(splits[3], (B, S), 0.1, 1.5, ((0, 4), (1, 8)), jnp.float32),
        "reward_mask": place_ends((jax.random.randint(splits[4], (B, S), 0, 4) < 1).astype(jnp.int32), jax.random.fold_in(splits[4], 1), 0, 1),
        "lengths": place_ends(jax.random.randint(splits[5], (B,), S // 4, S + 1), jax.random.fold_in(splits[5], 1), S // 4, S).astype(jnp.int32),
        "horizon": draw_horizon(jax.random.fold_in(splits[7], 71), 0),
    }


EPS = 1e-05

def reference(hidden, gain, value_weight, rewards, reward_mask, lengths, horizon):
    head_vec = gain * value_weight

    def head(rows):
        wide_rows = rows.astype(jnp.float32)
        return lax.optimization_barrier(jnp.sum(wide_rows * head_vec, -1)) * lax.rsqrt(lax.optimization_barrier(jnp.mean(wide_rows * wide_rows, -1)) + EPS)
    values = lax.map(head, hidden)
    length_all = hidden.shape[1]
    positions = jnp.arange(length_all, dtype=jnp.int32)
    valid = (positions[None, :] < lengths[:, None]).astype(jnp.float32)
    next_valid = (positions[None, :] + 1 < lengths[:, None]).astype(jnp.float32)
    next_values = jnp.concatenate([values[:, 1:], jnp.zeros((values.shape[0], 1), jnp.float32)], 1)
    delta = (rewards * reward_mask.astype(jnp.float32) + next_valid * next_values - values) * valid
    decay = jnp.exp(-1.0 / horizon)

    def step(carry, inputs):
        d_now, v_next = inputs
        fresh = d_now + decay * v_next * carry
        return (fresh, fresh)
    _, gae_t = lax.scan(step, jnp.zeros(values.shape[0], jnp.float32), (delta.T, next_valid.T), reverse=True)
    gae = gae_t.T
    returns = (gae + values) * valid
    count = jnp.sum(valid)
    first = jnp.sum(gae)
    second = jnp.sum(gae * gae)
    mean = first / count
    var = jnp.maximum(second / count - mean * mean, 1.0)
    advantages = (gae - mean) * valid * lax.rsqrt(var)
    return (advantages, returns)
```

```python
import functools

import jax
import jax.numpy as jnp
from jax import lax
from jax.experimental import pallas as pl
from jax.experimental.pallas import tpu as pltpu
from jax.sharding import PartitionSpec as P

EPS = 1e-05
LANES = 128
CHUNK_BYTES = 256 * 1024


def split_bf16(x, terms):
    out = []
    for _ in range(terms):
        top = x.astype(jnp.bfloat16)
        out.append(top)
        x = x - top.astype(jnp.float32)
    return out


def dot_nt(a, b):
    return lax.dot_general(a, b, (((1,), (1,)), ((), ())), preferred_element_type=jnp.float32)


def sums_kernel(hidden, gain, weight, rewards, mask, out, buf, sems, *, tokens, per_response):
    count, rows, width = buf.shape
    responses, block = rewards.shape
    copies = []
    for c in range(count):
        r, at = divmod(c * rows, tokens)
        copy = pltpu.make_async_copy(hidden.at[r, pl.ds(at, rows)], buf.at[c], sems.at[c])
        copy.start()
        copies.append(copy)
    head = split_bf16(gain[...] * weight[...], 3)
    index = lax.broadcasted_iota(jnp.int32, (8, width), 0)
    left = jnp.zeros((8, width), jnp.float32)
    for i, term in enumerate(head):
        left = jnp.where(index == i, term.astype(jnp.float32), left)
    left = left.astype(jnp.bfloat16)
    ones = jnp.where(lax.broadcasted_iota(jnp.int32, (8, LANES), 0) == 0, 1.0, 0.0).astype(jnp.bfloat16)
    base = 2 * responses * per_response
    out[pl.ds(base, responses * per_response), :] = jnp.zeros((responses * per_response, LANES), jnp.float32)
    here = lax.axis_index("seq") * (block // LANES)
    paid = rewards[...] * mask[...].astype(jnp.float32)
    for r in range(responses):
        for j in range(block // LANES):
            out[pl.ds(base + r * per_response + here + j, 1), :] = paid[r : r + 1, j * LANES : (j + 1) * LANES]
    for c in range(count):
        copies[c].wait()
        r, at = divmod(c * rows, tokens)
        h = buf[c]
        projected = jnp.sum(dot_nt(left, h), 0, keepdims=True)
        wide = h.astype(jnp.float32)
        wide = wide * wide
        folded = wide[:, :LANES]
        for k in range(1, width // LANES):
            folded = folded + wide[:, k * LANES : (k + 1) * LANES]
        high, low = split_bf16(folded, 2)
        squares = jnp.sum(dot_nt(ones, high) + dot_nt(ones, low), 0, keepdims=True)
        to = 2 * r * per_response + at // LANES
        for j in range(rows // LANES):
            out[pl.ds(to + j, 1), :] = squares[:, j * LANES : (j + 1) * LANES]
            out[pl.ds(to + per_response + j, 1), :] = projected[:, j * LANES : (j + 1) * LANES]


def gae_kernel(mine, other, lengths, horizon, out, gae_s, ret_s, *, features, block):
    responses = lengths.shape[0]
    R = gae_s.shape[1]
    rows = block // LANES
    row = lax.broadcasted_iota(jnp.int32, (R, LANES), 0)
    lane = lax.broadcasted_iota(jnp.int32, (R, LANES), 1)
    position = row * LANES + lane
    here = lax.axis_index("seq") * rows
    first = jnp.zeros((1, LANES), jnp.float32)
    second = jnp.zeros((1, LANES), jnp.float32)
    stats = rows * 2 * responses

    def part(i):
        at = pl.ds(i * R, R)
        return mine[at, :] + other[at, :]

    out[pl.ds(stats, 8), :] = jnp.zeros((8, LANES), jnp.float32)
    for r in range(responses):
        value = part(2 * r + 1) * lax.rsqrt(part(2 * r) / features + EPS)
        length = lengths[r]
        valid = (position < length).astype(jnp.float32)
        next_valid = (position + 1 < length).astype(jnp.float32)
        ahead = pltpu.roll(value, LANES - 1, 1)
        below = pltpu.roll(ahead, R - 1, 0)
        next_value = jnp.where(lane == LANES - 1, below, ahead)
        x = (part(2 * responses + r) + next_valid * next_value - value) * valid
        log_decay = -1.0 / jnp.full((1, LANES), horizon[r], jnp.float32)
        step = 1
        while step < LANES:
            moved = jnp.where(lane < LANES - step, pltpu.roll(x, LANES - step, 1), 0.0)
            x = x + jnp.exp(log_decay * step) * moved
            step *= 2
        start = jnp.broadcast_to(x[:, 0:1], (R, LANES))
        step = 1
        while step < R:
            moved = jnp.where(row < R - step, pltpu.roll(start, R - step, 0), 0.0)
            start = start + jnp.exp(log_decay * (step * LANES)) * moved
            step *= 2
        entering = jnp.where(row < R - 1, pltpu.roll(start, R - 1, 0), 0.0)
        gae = x + jnp.exp(log_decay * (LANES - lane).astype(jnp.float32)) * entering
        gae_s[r] = gae
        ret_s[r] = (gae + value) * valid
        first = first + jnp.sum(gae, 0, keepdims=True)
        second = second + jnp.sum(gae * gae, 0, keepdims=True)
        out[pl.ds(stats + 2 + r, 1), :] = jnp.full((1, LANES), length, jnp.int32).astype(jnp.float32)
        for j in range(rows):
            at = j * 2 * responses + r
            out[pl.ds(at, 1), :] = gae_s[r, pl.ds(here + j, 1), :]
            out[pl.ds(at + responses, 1), :] = ret_s[r, pl.ds(here + j, 1), :]
    out[pl.ds(stats, 1), :] = first
    out[pl.ds(stats + 1, 1), :] = second


def whiten_kernel(*refs, responses, block):
    parts, (adv, ret, rolled_s) = refs[:-3], refs[-3:]
    peers = len(parts)
    size = block // peers
    me = lax.axis_index("batch")
    rows = 2 * responses
    stats = (block // LANES) * rows
    offset = me * size
    for k, part in enumerate(parts):
        rolled_s[pl.ds(k * rows, rows), :] = part[pl.ds(offset // LANES * rows, rows), :]
    tokens = pltpu.roll(rolled_s[...], (LANES - offset % LANES) % LANES, 1)
    totals = parts[0][pl.ds(stats, 8), :]
    for part in parts[1:]:
        totals = totals + part[pl.ds(stats, 8), :]
    totals_sum = jnp.sum(totals[0:2], 1, keepdims=True)
    count = jnp.sum(totals[2 : 2 + responses, 0:1], 0, keepdims=True)
    mean = totals_sum[0:1] / count
    var = jnp.maximum(totals_sum[1:2] / count - mean * mean, 1.0)
    scale = lax.rsqrt(var)
    position = lax.axis_index("seq") * block + offset + lax.broadcasted_iota(jnp.int32, (responses, size), 1)
    for k, part in enumerate(parts):
        length = part[pl.ds(stats + 2, responses), :][:, :size]
        valid = (position.astype(jnp.float32) < length).astype(jnp.float32)
        to = pl.ds((me ^ k) * responses, responses)
        gae = tokens[k * rows : k * rows + responses, :size]
        adv[to, :] = (gae - mean) * valid * scale
        ret[to, :] = tokens[k * rows + responses : (k + 1) * rows, :size]


def exchange(x, axis, k):
    n = lax.axis_size(axis)
    return lax.ppermute(x, axis, [(i, i ^ k) for i in range(n)])


def vmem(n):
    return [pl.BlockSpec(memory_space=pltpu.VMEM)] * n


def per_device(hidden, gain, value_weight, rewards, reward_mask, lengths, horizon):
    responses, tokens, width = hidden.shape
    block = rewards.shape[1]
    n_seq, n_batch = lax.axis_size("seq"), lax.axis_size("batch")
    assert n_seq & (n_seq - 1) == 0 and n_batch & (n_batch - 1) == 0
    assert block % LANES == 0 and width % LANES == 0 and responses <= 6
    R = tokens // LANES
    chunk = min(max(LANES, CHUNK_BYTES // (2 * width)), tokens)
    while tokens % chunk:
        chunk -= LANES
    chunks = responses * tokens // chunk
    sums = pl.pallas_call(
        functools.partial(sums_kernel, tokens=tokens, per_response=R),
        out_shape=jax.ShapeDtypeStruct((3 * responses * R, LANES), jnp.float32),
        in_specs=[pl.BlockSpec(memory_space=pl.ANY)] + vmem(4),
        out_specs=vmem(1)[0],
        scratch_shapes=[
            pltpu.VMEM((chunks, chunk, width), jnp.bfloat16),
            pltpu.SemaphoreType.DMA((chunks,)),
        ],
        name="sums",
    )(hidden, gain[None], value_weight[None], rewards, reward_mask)
    k = 1
    other = jnp.zeros_like(sums)
    while k < n_seq:
        if k > 1:
            sums = sums + other
        other = exchange(sums, "seq", k)
        k *= 2
    payload_rows = (block // LANES) * 2 * responses + 8
    smem = pl.BlockSpec(memory_space=pltpu.SMEM)
    payload = pl.pallas_call(
        functools.partial(gae_kernel, features=width * n_seq, block=block),
        out_shape=jax.ShapeDtypeStruct((payload_rows, LANES), jnp.float32),
        in_specs=vmem(2) + [smem, smem],
        out_specs=vmem(1)[0],
        scratch_shapes=[pltpu.VMEM((responses, R, LANES), jnp.float32)] * 2,
        name="gae",
    )(sums, other, lengths, horizon)
    parts = [payload] + [exchange(payload, "batch", k) for k in range(1, n_batch)]
    shape = jax.ShapeDtypeStruct((responses * n_batch, block // n_batch), jnp.float32)
    return pl.pallas_call(
        functools.partial(whiten_kernel, responses=responses, block=block),
        out_shape=(shape, shape),
        in_specs=vmem(n_batch),
        out_specs=tuple(vmem(2)),
        scratch_shapes=[pltpu.VMEM((2 * responses * n_batch, LANES), jnp.float32)],
        name="whiten",
    )(*parts)


def solution(mesh):
    return jax.shard_map(
        per_device,
        mesh=mesh,
        in_specs=(
            P("batch", None, "seq"),
            P("seq"),
            P("seq"),
            P("batch", "seq"),
            P("batch", "seq"),
            P("batch"),
            P("batch"),
        ),
        out_specs=(P(None, ("seq", "batch")), P(None, ("seq", "batch"))),
        check_vma=False,
    )
```

```python
import functools

import jax
import jax.numpy as jnp
from jax import lax
from jax.experimental import pallas as pl
from jax.experimental.pallas import tpu as pltpu
from jax.sharding import PartitionSpec as P

EPS = 1e-05
LANES = 128
CHUNK_BYTES = 1024 * 1024


def split_bf16(x, terms):
    out = []
    for _ in range(terms):
        top = x.astype(jnp.bfloat16)
        out.append(top)
        x = x - top.astype(jnp.float32)
    return out


def dot_nt(a, b):
    return lax.dot_general(a, b, (((1,), (1,)), ((), ())), preferred_element_type=jnp.float32)


def sums_kernel(hidden, *refs, tokens, per_response):
    sources, out, buf, small, sems = refs[:4], refs[4], refs[5], refs[6:10], refs[10]
    gain, weight, rewards, mask = small
    count, rows, width = buf.shape
    responses, block = rewards.shape
    starts = [pltpu.make_async_copy(a, b, sems.at[count + i]) for i, (a, b) in enumerate(zip(sources, small))]
    for copy in starts:
        copy.start()
    copies = []
    for c in range(count):
        r, at = divmod(c * rows, tokens)
        copy = pltpu.make_async_copy(hidden.at[r, pl.ds(at, rows)], buf.at[c], sems.at[c])
        copy.start()
        copies.append(copy)
    for copy in starts:
        copy.wait()
    head = split_bf16(gain[...] * weight[...], 3)
    index = lax.broadcasted_iota(jnp.int32, (8, width), 0)
    left = jnp.zeros((8, width), jnp.float32)
    for i, term in enumerate(head):
        left = jnp.where(index == i, term.astype(jnp.float32), left)
    left = left.astype(jnp.bfloat16)
    ones = jnp.where(lax.broadcasted_iota(jnp.int32, (8, LANES), 0) == 0, 1.0, 0.0).astype(jnp.bfloat16)
    base = 2 * responses * per_response
    out[pl.ds(base, responses * per_response), :] = jnp.zeros((responses * per_response, LANES), jnp.float32)
    here = lax.axis_index("seq") * (block // LANES)
    paid = rewards[...] * mask[...].astype(jnp.float32)
    for r in range(responses):
        for j in range(block // LANES):
            out[pl.ds(base + r * per_response + here + j, 1), :] = paid[r : r + 1, j * LANES : (j + 1) * LANES]
    for c in range(count):
        copies[c].wait()
        r, at = divmod(c * rows, tokens)
        h = buf[c]
        projected = jnp.sum(dot_nt(left, h), 0, keepdims=True)
        wide = h.astype(jnp.float32)
        wide = wide * wide
        folded = wide[:, :LANES]
        for k in range(1, width // LANES):
            folded = folded + wide[:, k * LANES : (k + 1) * LANES]
        high, low = split_bf16(folded, 2)
        squares = jnp.sum(dot_nt(ones, high) + dot_nt(ones, low), 0, keepdims=True)
        to = 2 * r * per_response + at // LANES
        for j in range(rows // LANES):
            out[pl.ds(to + j, 1), :] = squares[:, j * LANES : (j + 1) * LANES]
            out[pl.ds(to + per_response + j, 1), :] = projected[:, j * LANES : (j + 1) * LANES]


def gae_kernel(mine, other, lengths, horizon, out, gae_s, ret_s, *, features, block):
    responses = lengths.shape[0]
    R = gae_s.shape[1]
    rows = block // LANES
    row = lax.broadcasted_iota(jnp.int32, (R, LANES), 0)
    lane = lax.broadcasted_iota(jnp.int32, (R, LANES), 1)
    position = row * LANES + lane
    here = lax.axis_index("seq") * rows
    first = jnp.zeros((1, LANES), jnp.float32)
    second = jnp.zeros((1, LANES), jnp.float32)
    stats = rows * 2 * responses

    def part(i):
        at = pl.ds(i * R, R)
        return mine[at, :] + other[at, :]

    out[pl.ds(stats, 8), :] = jnp.zeros((8, LANES), jnp.float32)
    for r in range(responses):
        value = part(2 * r + 1) * lax.rsqrt(part(2 * r) / features + EPS)
        length = lengths[r]
        valid = (position < length).astype(jnp.float32)
        next_valid = (position + 1 < length).astype(jnp.float32)
        ahead = pltpu.roll(value, LANES - 1, 1)
        below = pltpu.roll(ahead, R - 1, 0)
        next_value = jnp.where(lane == LANES - 1, below, ahead)
        x = (part(2 * responses + r) + next_valid * next_value - value) * valid
        log_decay = -1.0 / jnp.full((1, LANES), horizon[r], jnp.float32)
        step = 1
        while step < LANES:
            moved = jnp.where(lane < LANES - step, pltpu.roll(x, LANES - step, 1), 0.0)
            x = x + jnp.exp(log_decay * step) * moved
            step *= 2
        start = jnp.broadcast_to(x[:, 0:1], (R, LANES))
        step = 1
        while step < R:
            moved = jnp.where(row < R - step, pltpu.roll(start, R - step, 0), 0.0)
            start = start + jnp.exp(log_decay * (step * LANES)) * moved
            step *= 2
        entering = jnp.where(row < R - 1, pltpu.roll(start, R - 1, 0), 0.0)
        gae = x + jnp.exp(log_decay * (LANES - lane).astype(jnp.float32)) * entering
        gae_s[r] = gae
        ret_s[r] = (gae + value) * valid
        first = first + jnp.sum(gae, 0, keepdims=True)
        second = second + jnp.sum(gae * gae, 0, keepdims=True)
        out[pl.ds(stats + 2 + r, 1), :] = jnp.full((1, LANES), length, jnp.int32).astype(jnp.float32)
        for j in range(rows):
            at = j * 2 * responses + r
            out[pl.ds(at, 1), :] = gae_s[r, pl.ds(here + j, 1), :]
            out[pl.ds(at + responses, 1), :] = ret_s[r, pl.ds(here + j, 1), :]
    out[pl.ds(stats, 1), :] = first
    out[pl.ds(stats + 1, 1), :] = second


def whiten_kernel(*refs, responses, block):
    parts, (adv, ret, rolled_s) = refs[:-3], refs[-3:]
    peers = len(parts)
    size = block // peers
    me = lax.axis_index("batch")
    rows = 2 * responses
    stats = (block // LANES) * rows
    offset = me * size
    for k, part in enumerate(parts):
        rolled_s[pl.ds(k * rows, rows), :] = part[pl.ds(offset // LANES * rows, rows), :]
    tokens = pltpu.roll(rolled_s[...], (LANES - offset % LANES) % LANES, 1)
    totals = parts[0][pl.ds(stats, 8), :]
    for part in parts[1:]:
        totals = totals + part[pl.ds(stats, 8), :]
    totals_sum = jnp.sum(totals[0:2], 1, keepdims=True)
    count = jnp.sum(totals[2 : 2 + responses, 0:1], 0, keepdims=True)
    mean = totals_sum[0:1] / count
    var = jnp.maximum(totals_sum[1:2] / count - mean * mean, 1.0)
    scale = lax.rsqrt(var)
    position = lax.axis_index("seq") * block + offset + lax.broadcasted_iota(jnp.int32, (responses, size), 1)
    for k, part in enumerate(parts):
        length = part[pl.ds(stats + 2, responses), :][:, :size]
        valid = (position.astype(jnp.float32) < length).astype(jnp.float32)
        to = pl.ds((me ^ k) * responses, responses)
        gae = tokens[k * rows : k * rows + responses, :size]
        adv[to, :] = (gae - mean) * valid * scale
        ret[to, :] = tokens[k * rows + responses : (k + 1) * rows, :size]


def exchange(x, axis, k):
    n = lax.axis_size(axis)
    return lax.ppermute(x, axis, [(i, i ^ k) for i in range(n)])


def vmem(n):
    return [pl.BlockSpec(memory_space=pltpu.VMEM)] * n


def per_device(hidden, gain, value_weight, rewards, reward_mask, lengths, horizon):
    responses, tokens, width = hidden.shape
    block = rewards.shape[1]
    n_seq, n_batch = lax.axis_size("seq"), lax.axis_size("batch")
    assert n_seq & (n_seq - 1) == 0 and n_batch & (n_batch - 1) == 0
    assert block % LANES == 0 and width % LANES == 0 and responses <= 6
    R = tokens // LANES
    chunk = min(max(LANES, CHUNK_BYTES // (2 * width)), tokens)
    while tokens % chunk:
        chunk -= LANES
    chunks = responses * tokens // chunk
    sums = pl.pallas_call(
        functools.partial(sums_kernel, tokens=tokens, per_response=R),
        out_shape=pltpu.VMEM((3 * responses * R, LANES), jnp.float32),
        in_specs=[pl.BlockSpec(memory_space=pltpu.HBM)] * 5,
        out_specs=vmem(1)[0],
        scratch_shapes=[
            pltpu.VMEM((chunks, chunk, width), jnp.bfloat16),
            pltpu.VMEM((1, width), jnp.float32),
            pltpu.VMEM((1, width), jnp.float32),
            pltpu.VMEM((responses, block), jnp.float32),
            pltpu.VMEM((responses, block), jnp.int32),
            pltpu.SemaphoreType.DMA((chunks + 4,)),
        ],
        name="sums",
    )(hidden, gain[None], value_weight[None], rewards, reward_mask)
    k = 1
    other = jnp.zeros_like(sums)
    while k < n_seq:
        if k > 1:
            sums = sums + other
        other = exchange(sums, "seq", k)
        k *= 2
    payload_rows = (block // LANES) * 2 * responses + 8
    smem = pl.BlockSpec(memory_space=pltpu.SMEM)
    payload = pl.pallas_call(
        functools.partial(gae_kernel, features=width * n_seq, block=block),
        out_shape=jax.ShapeDtypeStruct((payload_rows, LANES), jnp.float32),
        in_specs=vmem(2) + [smem, smem],
        out_specs=vmem(1)[0],
        scratch_shapes=[pltpu.VMEM((responses, R, LANES), jnp.float32)] * 2,
        compiler_params=pltpu.CompilerParams(vmem_limit_bytes=4 * 1024 * 1024),
        name="gae",
    )(sums, other, lengths, horizon)
    parts = [payload] + [exchange(payload, "batch", k) for k in range(1, n_batch)]
    shape = jax.ShapeDtypeStruct((responses * n_batch, block // n_batch), jnp.float32)
    return pl.pallas_call(
        functools.partial(whiten_kernel, responses=responses, block=block),
        out_shape=(shape, shape),
        in_specs=vmem(n_batch),
        out_specs=tuple(vmem(2)),
        scratch_shapes=[pltpu.VMEM((2 * responses * n_batch, LANES), jnp.float32)],
        compiler_params=pltpu.CompilerParams(vmem_limit_bytes=4 * 1024 * 1024),
        name="whiten",
    )(*parts)


def solution(mesh):
    return jax.shard_map(
        per_device,
        mesh=mesh,
        in_specs=(
            P("batch", None, "seq"),
            P("seq"),
            P("seq"),
            P("batch", "seq"),
            P("batch", "seq"),
            P("batch"),
            P("batch"),
        ),
        out_specs=(P(None, ("seq", "batch")), P(None, ("seq", "batch"))),
        check_vma=False,
    )
```

```python
import functools

import jax
import jax.numpy as jnp
from jax import lax
from jax.experimental import pallas as pl
from jax.experimental.pallas import tpu as pltpu
from jax.sharding import PartitionSpec as P

EPS = 1e-05
LANES = 128
CHUNK_BYTES = 1024 * 1024


def split_bf16(x, terms):
    out = []
    for _ in range(terms):
        top = x.astype(jnp.bfloat16)
        out.append(top)
        x = x - top.astype(jnp.float32)
    return out


def dot_nt(a, b):
    return lax.dot_general(a, b, (((1,), (1,)), ((), ())), preferred_element_type=jnp.float32)


def sums_kernel(hidden, *refs, tokens, per_response):
    sources, out, buf, small, sems = refs[:6], refs[6], refs[7], refs[8:14], refs[14]
    gain, weight, rewards, mask, lengths, horizon = small
    count, rows, width = buf.shape
    responses, block = rewards.shape
    starts = [pltpu.make_async_copy(a, b, sems.at[count + i]) for i, (a, b) in enumerate(zip(sources, small))]
    for copy in starts:
        copy.start()
    copies = []
    for c in range(count):
        r, at = divmod(c * rows, tokens)
        copy = pltpu.make_async_copy(hidden.at[r, pl.ds(at, rows)], buf.at[c], sems.at[c])
        copy.start()
        copies.append(copy)
    for copy in starts:
        copy.wait()
    head = split_bf16(gain[...] * weight[...], 3)
    index = lax.broadcasted_iota(jnp.int32, (8, width), 0)
    left = jnp.zeros((8, width), jnp.float32)
    for i, term in enumerate(head):
        left = jnp.where(index == i, term.astype(jnp.float32), left)
    left = left.astype(jnp.bfloat16)
    ones = jnp.where(lax.broadcasted_iota(jnp.int32, (8, LANES), 0) == 0, 1.0, 0.0).astype(jnp.bfloat16)
    base = 2 * responses * per_response
    out[pl.ds(base, responses * per_response), :] = jnp.zeros((responses * per_response, LANES), jnp.float32)
    info = base + responses * per_response
    for r in range(responses):
        out[pl.ds(info + r, 1), :] = jnp.full((1, LANES), lengths[r], jnp.int32).astype(jnp.float32)
        out[pl.ds(info + responses + r, 1), :] = jnp.full((1, LANES), horizon[r], jnp.float32)
    here = lax.axis_index("seq") * (block // LANES)
    paid = rewards[...] * mask[...].astype(jnp.float32)
    for r in range(responses):
        for j in range(block // LANES):
            out[pl.ds(base + r * per_response + here + j, 1), :] = paid[r : r + 1, j * LANES : (j + 1) * LANES]
    for c in range(count):
        copies[c].wait()
        r, at = divmod(c * rows, tokens)
        h = buf[c]
        projected = jnp.sum(dot_nt(left, h), 0, keepdims=True)
        wide = h.astype(jnp.float32)
        wide = wide * wide
        folded = wide[:, :LANES]
        for k in range(1, width // LANES):
            folded = folded + wide[:, k * LANES : (k + 1) * LANES]
        high, low = split_bf16(folded, 2)
        squares = jnp.sum(dot_nt(ones, high) + dot_nt(ones, low), 0, keepdims=True)
        to = 2 * r * per_response + at // LANES
        for j in range(rows // LANES):
            out[pl.ds(to + j, 1), :] = squares[:, j * LANES : (j + 1) * LANES]
            out[pl.ds(to + per_response + j, 1), :] = projected[:, j * LANES : (j + 1) * LANES]


def gae_kernel(mine, other, theirs, ours, out, gae_s, ret_s, *, features, block):
    total, R, _ = gae_s.shape
    responses = total // 2
    rows = block // LANES
    row = lax.broadcasted_iota(jnp.int32, (R, LANES), 0)
    lane = lax.broadcasted_iota(jnp.int32, (R, LANES), 1)
    position = (row * LANES + lane).astype(jnp.float32)
    here = lax.axis_index("seq") * rows
    first = jnp.zeros((1, LANES), jnp.float32)
    second = jnp.zeros((1, LANES), jnp.float32)
    stats = rows * 2 * total
    info = 3 * responses * R

    for g in range(total):
        core, r = divmod(g, responses)
        held = (theirs, ours)[core]

        def part(i):
            at = pl.ds((core * 3 * responses + i) * R, R)
            return mine[at, :] + other[at, :]

        value = part(2 * r + 1) * lax.rsqrt(part(2 * r) / features + EPS)
        length = held[pl.ds(info + r, 1), :]
        valid = (position < length).astype(jnp.float32)
        next_valid = (position + 1.0 < length).astype(jnp.float32)
        ahead = pltpu.roll(value, LANES - 1, 1)
        below = pltpu.roll(ahead, R - 1, 0)
        next_value = jnp.where(lane == LANES - 1, below, ahead)
        x = (part(2 * responses + r) + next_valid * next_value - value) * valid
        log_decay = -1.0 / held[pl.ds(info + responses + r, 1), :]
        step = 1
        while step < LANES:
            moved = jnp.where(lane < LANES - step, pltpu.roll(x, LANES - step, 1), 0.0)
            x = x + jnp.exp(log_decay * step) * moved
            step *= 2
        start = jnp.broadcast_to(x[:, 0:1], (R, LANES))
        step = 1
        while step < R:
            moved = jnp.where(row < R - step, pltpu.roll(start, R - step, 0), 0.0)
            start = start + jnp.exp(log_decay * (step * LANES)) * moved
            step *= 2
        entering = jnp.where(row < R - 1, pltpu.roll(start, R - 1, 0), 0.0)
        gae = x + jnp.exp(log_decay * (LANES - lane).astype(jnp.float32)) * entering
        gae_s[g] = gae
        ret_s[g] = (gae + value) * valid
        first = first + jnp.sum(gae, 0, keepdims=True)
        second = second + jnp.sum(gae * gae, 0, keepdims=True)
        out[pl.ds(stats + 2 + g, 1), :] = length
    for g in range(total):
        for j in range(rows):
            at = j * 2 * total + g
            out[pl.ds(at, 1), :] = gae_s[g, pl.ds(here + j, 1), :]
            out[pl.ds(at + total, 1), :] = ret_s[g, pl.ds(here + j, 1), :]
    out[pl.ds(stats, 1), :] = first
    out[pl.ds(stats + 1, 1), :] = second


def whiten_kernel(*refs, total, block):
    pairs, (adv, ret, parts, rolled_s) = refs[:-4], refs[-4:]
    chips = len(pairs) // 2
    size = block // lax.axis_size("batch")
    me = lax.axis_index("batch")
    rows = 2 * total
    stats = (block // LANES) * rows
    offset = me * size
    for k in range(chips):
        parts[k] = jnp.where(me % 2 == 1, pairs[2 * k][...], pairs[2 * k + 1][...])
        rolled_s[pl.ds(k * rows, rows), :] = parts[k, pl.ds(offset // LANES * rows, rows), :]
    tokens = pltpu.roll(rolled_s[...], (LANES - offset % LANES) % LANES, 1)
    totals = parts[0, pl.ds(stats, 2 + total), :]
    for k in range(1, chips):
        totals = totals + parts[k, pl.ds(stats, 2 + total), :]
    totals_sum = jnp.sum(totals[0:2], 1, keepdims=True)
    count = jnp.sum(totals[2 : 2 + total, 0:1], 0, keepdims=True)
    mean = totals_sum[0:1] / count
    var = jnp.maximum(totals_sum[1:2] / count - mean * mean, 1.0)
    scale = lax.rsqrt(var)
    position = lax.axis_index("seq") * block + offset + lax.broadcasted_iota(jnp.int32, (total, size), 1)
    for k in range(chips):
        length = parts[k, pl.ds(stats + 2, total), :][:, :size]
        valid = (position.astype(jnp.float32) < length).astype(jnp.float32)
        to = pl.ds(((me // 2) ^ k) * total, total)
        gae = tokens[k * rows : k * rows + total, :size]
        adv[to, :] = (gae - mean) * valid * scale
        ret[to, :] = tokens[k * rows + total : (k + 1) * rows, :size]


def send(x, seq_step, chip_step, source_core, target_core):
    n_seq, chips = lax.axis_size("seq"), lax.axis_size("batch") // 2
    pairs = []
    for s in range(n_seq):
        for c in range(chips):
            source = (s * chips + c) * 2 + source_core
            target = ((s ^ seq_step) * chips + (c ^ chip_step)) * 2 + target_core
            pairs.append((source, target))
    return lax.ppermute(x, ("seq", "batch"), pairs)


def vmem(n):
    return [pl.BlockSpec(memory_space=pltpu.VMEM)] * n


def per_device(hidden, gain, value_weight, rewards, reward_mask, lengths, horizon):
    responses, tokens, width = hidden.shape
    block = rewards.shape[1]
    n_seq, n_batch = lax.axis_size("seq"), lax.axis_size("batch")
    assert n_seq & (n_seq - 1) == 0 and n_batch & (n_batch - 1) == 0
    assert block % LANES == 0 and width % LANES == 0 and responses <= 3 and n_batch > 1
    R = tokens // LANES
    chunk = min(max(LANES, CHUNK_BYTES // (2 * width)), tokens)
    while tokens % chunk:
        chunk -= LANES
    chunks = responses * tokens // chunk
    sums = pl.pallas_call(
        functools.partial(sums_kernel, tokens=tokens, per_response=R),
        out_shape=pltpu.VMEM((3 * responses * R + 8, LANES), jnp.float32),
        in_specs=[pl.BlockSpec(memory_space=pltpu.HBM)] * 7,
        out_specs=vmem(1)[0],
        scratch_shapes=[
            pltpu.VMEM((chunks, chunk, width), jnp.bfloat16),
            pltpu.VMEM((1, width), jnp.float32),
            pltpu.VMEM((1, width), jnp.float32),
            pltpu.VMEM((responses, block), jnp.float32),
            pltpu.VMEM((responses, block), jnp.int32),
            pltpu.SMEM((responses,), jnp.int32),
            pltpu.SMEM((responses,), jnp.float32),
            pltpu.SemaphoreType.DMA((chunks + 6,)),
        ],
        name="sums",
    )(hidden, gain[None], value_weight[None], rewards, reward_mask, lengths, horizon)
    theirs = send(sums, 0, 0, 0, 1)
    both = jnp.concatenate([theirs[: 3 * responses * R], sums[: 3 * responses * R]], 0)
    k = 1
    other = jnp.zeros_like(both)
    while k < n_seq:
        if k > 1:
            both = both + other
        other = send(both, k, 0, 1, 1)
        k *= 2
    total = 2 * responses
    payload_rows = (block // LANES) * 2 * total + 8
    limit = pltpu.CompilerParams(vmem_limit_bytes=4 * 1024 * 1024)
    payload = pl.pallas_call(
        functools.partial(gae_kernel, features=width * n_seq, block=block),
        out_shape=jax.ShapeDtypeStruct((payload_rows, LANES), jnp.float32),
        in_specs=vmem(4),
        out_specs=vmem(1)[0],
        scratch_shapes=[pltpu.VMEM((total, R, LANES), jnp.float32)] * 2,
        compiler_params=limit,
        name="gae",
    )(both, other, theirs, sums)
    chips = n_batch // 2
    pairs = [payload, send(payload, 0, 0, 1, 0)]
    for k in range(1, chips):
        pairs += [send(payload, 0, k, 1, 1), send(payload, 0, k, 1, 0)]
    shape = jax.ShapeDtypeStruct((responses * n_batch, block // n_batch), jnp.float32)
    return pl.pallas_call(
        functools.partial(whiten_kernel, total=total, block=block),
        out_shape=(shape, shape),
        in_specs=vmem(2 * chips),
        out_specs=tuple(vmem(2)),
        scratch_shapes=[
            pltpu.VMEM((chips, payload_rows, LANES), jnp.float32),
            pltpu.VMEM((2 * total * chips, LANES), jnp.float32),
        ],
        compiler_params=limit,
        name="whiten",
    )(*pairs)


def solution(mesh):
    return jax.shard_map(
        per_device,
        mesh=mesh,
        in_specs=(
            P("batch", None, "seq"),
            P("seq"),
            P("seq"),
            P("batch", "seq"),
            P("batch", "seq"),
            P("batch"),
            P("batch"),
        ),
        out_specs=(P(None, ("seq", "batch")), P(None, ("seq", "batch"))),
        check_vma=False,
    )
```

```python
import functools

import jax
import jax.numpy as jnp
from jax import lax
from jax.experimental import pallas as pl
from jax.experimental.pallas import tpu as pltpu
from jax.sharding import PartitionSpec as P

EPS = 1e-05
LANES = 128
CHUNK_BYTES = 1024 * 1024


def split_bf16(x, terms):
    out = []
    for _ in range(terms):
        top = x.astype(jnp.bfloat16)
        out.append(top)
        x = x - top.astype(jnp.float32)
    return out


def dot_nt(a, b):
    return lax.dot_general(a, b, (((1,), (1,)), ((), ())), preferred_element_type=jnp.float32)


def sums_kernel(hidden, *refs, tokens, per_response):
    sources, out, buf, small, sems = refs[:4], refs[4], refs[5], refs[6:10], refs[10]
    gain, weight, rewards, mask = small
    count, rows, width = buf.shape
    responses, block = rewards.shape
    starts = [pltpu.make_async_copy(a, b, sems.at[count + i]) for i, (a, b) in enumerate(zip(sources, small))]
    for copy in starts:
        copy.start()
    copies = []
    for c in range(count):
        r, at = divmod(c * rows, tokens)
        copy = pltpu.make_async_copy(hidden.at[r, pl.ds(at, rows)], buf.at[c], sems.at[c])
        copy.start()
        copies.append(copy)
    for copy in starts:
        copy.wait()
    head = split_bf16(gain[...] * weight[...], 3)
    index = lax.broadcasted_iota(jnp.int32, (8, width), 0)
    left = jnp.zeros((8, width), jnp.float32)
    for i, term in enumerate(head):
        left = jnp.where(index == i, term.astype(jnp.float32), left)
    left = left.astype(jnp.bfloat16)
    ones = jnp.where(lax.broadcasted_iota(jnp.int32, (8, LANES), 0) == 0, 1.0, 0.0).astype(jnp.bfloat16)
    base = 2 * responses * per_response
    out[pl.ds(base, responses * per_response), :] = jnp.zeros((responses * per_response, LANES), jnp.float32)
    here = lax.axis_index("seq") * (block // LANES)
    paid = rewards[...] * mask[...].astype(jnp.float32)
    for r in range(responses):
        for j in range(block // LANES):
            out[pl.ds(base + r * per_response + here + j, 1), :] = paid[r : r + 1, j * LANES : (j + 1) * LANES]
    for c in range(count):
        copies[c].wait()
        r, at = divmod(c * rows, tokens)
        h = buf[c]
        projected = jnp.sum(dot_nt(left, h), 0, keepdims=True)
        wide = h.astype(jnp.float32)
        wide = wide * wide
        folded = wide[:, :LANES]
        for k in range(1, width // LANES):
            folded = folded + wide[:, k * LANES : (k + 1) * LANES]
        high, low = split_bf16(folded, 2)
        squares = jnp.sum(dot_nt(ones, high) + dot_nt(ones, low), 0, keepdims=True)
        to = 2 * r * per_response + at // LANES
        for j in range(rows // LANES):
            out[pl.ds(to + j, 1), :] = squares[:, j * LANES : (j + 1) * LANES]
            out[pl.ds(to + per_response + j, 1), :] = projected[:, j * LANES : (j + 1) * LANES]


def gae_kernel(mine, other, lengths, horizon, out, gae_s, ret_s, *, features, block):
    responses = lengths.shape[0]
    R = gae_s.shape[1]
    rows = block // LANES
    row = lax.broadcasted_iota(jnp.int32, (R, LANES), 0)
    lane = lax.broadcasted_iota(jnp.int32, (R, LANES), 1)
    position = row * LANES + lane
    here = lax.axis_index("seq") * rows
    first = jnp.zeros((1, LANES), jnp.float32)
    second = jnp.zeros((1, LANES), jnp.float32)
    stats = rows * 2 * responses

    def part(i):
        at = pl.ds(i * R, R)
        return mine[at, :] + other[at, :]

    out[pl.ds(stats, 8), :] = jnp.zeros((8, LANES), jnp.float32)
    for r in range(responses):
        value = part(2 * r + 1) * lax.rsqrt(part(2 * r) / features + EPS)
        length = lengths[r]
        valid = (position < length).astype(jnp.float32)
        next_valid = (position + 1 < length).astype(jnp.float32)
        ahead = pltpu.roll(value, LANES - 1, 1)
        below = pltpu.roll(ahead, R - 1, 0)
        next_value = jnp.where(lane == LANES - 1, below, ahead)
        x = (part(2 * responses + r) + next_valid * next_value - value) * valid
        log_decay = -1.0 / jnp.full((1, LANES), horizon[r], jnp.float32)
        step = 1
        while step < LANES:
            moved = jnp.where(lane < LANES - step, pltpu.roll(x, LANES - step, 1), 0.0)
            x = x + jnp.exp(log_decay * step) * moved
            step *= 2
        start = jnp.broadcast_to(x[:, 0:1], (R, LANES))
        step = 1
        while step < R:
            moved = jnp.where(row < R - step, pltpu.roll(start, R - step, 0), 0.0)
            start = start + jnp.exp(log_decay * (step * LANES)) * moved
            step *= 2
        entering = jnp.where(row < R - 1, pltpu.roll(start, R - 1, 0), 0.0)
        gae = x + jnp.exp(log_decay * (LANES - lane).astype(jnp.float32)) * entering
        gae_s[r] = gae
        ret_s[r] = (gae + value) * valid
        first = first + jnp.sum(gae, 0, keepdims=True)
        second = second + jnp.sum(gae * gae, 0, keepdims=True)
        out[pl.ds(stats + 2 + r, 1), :] = jnp.full((1, LANES), length, jnp.int32).astype(jnp.float32)
        for j in range(rows):
            at = j * 2 * responses + r
            out[pl.ds(at, 1), :] = gae_s[r, pl.ds(here + j, 1), :]
            out[pl.ds(at + responses, 1), :] = ret_s[r, pl.ds(here + j, 1), :]
    out[pl.ds(stats, 1), :] = first
    out[pl.ds(stats + 1, 1), :] = second


def whiten_kernel(*refs, responses, block):
    parts, (adv, ret, rolled_s) = refs[:-3], refs[-3:]
    peers = len(parts)
    size = block // peers
    me = lax.axis_index("batch")
    rows = 2 * responses
    stats = (block // LANES) * rows
    offset = me * size
    for k, part in enumerate(parts):
        rolled_s[pl.ds(k * rows, rows), :] = part[pl.ds(offset // LANES * rows, rows), :]
    tokens = pltpu.roll(rolled_s[...], (LANES - offset % LANES) % LANES, 1)
    totals = parts[0][pl.ds(stats, 8), :]
    for part in parts[1:]:
        totals = totals + part[pl.ds(stats, 8), :]
    totals_sum = jnp.sum(totals[0:2], 1, keepdims=True)
    count = jnp.sum(totals[2 : 2 + responses, 0:1], 0, keepdims=True)
    mean = totals_sum[0:1] / count
    var = jnp.maximum(totals_sum[1:2] / count - mean * mean, 1.0)
    scale = lax.rsqrt(var)
    position = lax.axis_index("seq") * block + offset + lax.broadcasted_iota(jnp.int32, (responses, size), 1)
    for k, part in enumerate(parts):
        length = part[pl.ds(stats + 2, responses), :][:, :size]
        valid = (position.astype(jnp.float32) < length).astype(jnp.float32)
        to = pl.ds((me ^ k) * responses, responses)
        gae = tokens[k * rows : k * rows + responses, :size]
        adv[to, :] = (gae - mean) * valid * scale
        ret[to, :] = tokens[k * rows + responses : (k + 1) * rows, :size]


def exchange(x, axis, k):
    n = lax.axis_size(axis)
    return lax.ppermute(x, axis, [(i, i ^ k) for i in range(n)])


def vmem(n):
    return [pl.BlockSpec(memory_space=pltpu.VMEM)] * n


def per_device(hidden, gain, value_weight, rewards, reward_mask, lengths, horizon):
    responses, tokens, width = hidden.shape
    block = rewards.shape[1]
    n_seq, n_batch = lax.axis_size("seq"), lax.axis_size("batch")
    assert n_seq & (n_seq - 1) == 0 and n_batch & (n_batch - 1) == 0
    assert block % LANES == 0 and width % LANES == 0 and responses <= 6
    R = tokens // LANES
    chunk = min(max(LANES, CHUNK_BYTES // (2 * width)), tokens)
    while tokens % chunk:
        chunk -= LANES
    chunks = responses * tokens // chunk
    sums = pl.pallas_call(
        functools.partial(sums_kernel, tokens=tokens, per_response=R),
        out_shape=pltpu.VMEM((3 * responses * R, LANES), jnp.float32),
        in_specs=[pl.BlockSpec(memory_space=pltpu.HBM)] * 5,
        out_specs=vmem(1)[0],
        scratch_shapes=[
            pltpu.VMEM((chunks, chunk, width), jnp.bfloat16),
            pltpu.VMEM((1, width), jnp.float32),
            pltpu.VMEM((1, width), jnp.float32),
            pltpu.VMEM((responses, block), jnp.float32),
            pltpu.VMEM((responses, block), jnp.int32),
            pltpu.SemaphoreType.DMA((chunks + 4,)),
        ],
        name="sums",
    )(hidden, gain[None], value_weight[None], rewards, reward_mask)
    k = 1
    other = jnp.zeros_like(sums)
    while k < n_seq:
        if k > 1:
            sums = sums + other
        other = exchange(sums, "seq", k + k // 2 if k > 1 and 2 * k == n_seq else k)
        k *= 2
    payload_rows = (block // LANES) * 2 * responses + 8
    smem = pl.BlockSpec(memory_space=pltpu.SMEM)
    payload = pl.pallas_call(
        functools.partial(gae_kernel, features=width * n_seq, block=block),
        out_shape=jax.ShapeDtypeStruct((payload_rows, LANES), jnp.float32),
        in_specs=vmem(2) + [smem, smem],
        out_specs=vmem(1)[0],
        scratch_shapes=[pltpu.VMEM((responses, R, LANES), jnp.float32)] * 2,
        compiler_params=pltpu.CompilerParams(vmem_limit_bytes=4 * 1024 * 1024),
        name="gae",
    )(sums, other, lengths, horizon)
    parts = [payload] + [exchange(payload, "batch", k) for k in range(1, n_batch)]
    shape = jax.ShapeDtypeStruct((responses * n_batch, block // n_batch), jnp.float32)
    return pl.pallas_call(
        functools.partial(whiten_kernel, responses=responses, block=block),
        out_shape=(shape, shape),
        in_specs=vmem(n_batch),
        out_specs=tuple(vmem(2)),
        scratch_shapes=[pltpu.VMEM((2 * responses * n_batch, LANES), jnp.float32)],
        compiler_params=pltpu.CompilerParams(vmem_limit_bytes=4 * 1024 * 1024),
        name="whiten",
    )(*parts)


def solution(mesh):
    return jax.shard_map(
        per_device,
        mesh=mesh,
        in_specs=(
            P("batch", None, "seq"),
            P("seq"),
            P("seq"),
            P("batch", "seq"),
            P("batch", "seq"),
            P("batch"),
            P("batch"),
        ),
        out_specs=(P(None, ("seq", "batch")), P(None, ("seq", "batch"))),
        check_vma=False,
    )
```
